256 devices in a mesh: slab: 32 (over z, x_hi, core), ang: 8 (over x_lo, y).
Axes of the slice: x: 4 (x_hi: 2, x_lo: 2; x = x_hi * 2 + x_lo), y: 4, z: 8, core: 2. Of those that a mesh axis runs over, the one named last changes fastest.
Arguments:
- volume: float32 [256, 256, 4096], P('slab', 'ang'), may hold values from 0.1 to 3
- measured: bfloat16 [8, 1024, 4096], P('ang', 'slab'), may hold values from 0 to 2
- foot_start: int32 [32, 8], P('slab', 'ang'), may hold values from 0 to 992, as said below
- foot_len: int32 [32, 8], P('slab', 'ang'), may hold values from 32 to 96
- order: int32 [64], replicated, may hold values from 0 to 63, each once
- ray_table: float32 [64, 256], replicated, may hold values from 0.001953125 to 0.0078125
Outputs:
- updated: float32 [256, 256, 4096], P('slab', 'ang')
- residual: float32 [8, 1024, 4096], P('ang', 'slab')
The draws below stay inside these ranges and needn't reach their ends.
Inputs may be any that keep to these rules, and one draw needn't show every extreme that they name: foot_start[s, j] + foot_len[s, j] <= 1024; the footprint of slab s lies within rows (s - 2) * 32 to (s + 3) * 32.
All inputs are finite; a program needn't handle non-finite values.
Results may differ from the reference program's by a relative error of at most 0.0003.
Values sent between devices are 32-bit elements; how exact they have to be, the bound alone decides.
A program may use at most 64 MiB of HBM per device.

```python
import math
import jax
import jax.numpy as jnp
from jax import lax

ZDEV = 8
NY = 256
NU = 4096
RDEV = 32
ANGLES = 8
ALL_ANG = 64
NZ = 256
NR = 1024
N_SLAB = 32


def footprint(key):
    base = jax.random.fold_in(key, 7)
    first_key, second_key = jax.random.split(base)
    slab_ids = jnp.arange(N_SLAB, dtype=jnp.int32)[:, None]
    spread = 2 * RDEV * jnp.abs(2 * slab_ids + 1 - N_SLAB) // (2 * N_SLAB)
    lengths = RDEV + spread + jax.random.randint(first_key, (N_SLAB, ANGLES), 0, RDEV + 1, dtype=jnp.int32)
    lengths = jnp.minimum(lengths, 3 * RDEV)
    jitter = jax.random.randint(second_key, (N_SLAB, ANGLES), -(RDEV // 2), RDEV // 2 + 1, dtype=jnp.int32)
    centre = slab_ids * RDEV + RDEV // 2 + jitter
    starts = jnp.clip(centre - lengths // 2, 0, RDEV * N_SLAB - lengths)
    return (starts.astype(jnp.int32), lengths.astype(jnp.int32))


def draw_foot_start(key, part):
    return footprint(key)[0]


def draw_foot_len(key, part):
    return footprint(key)[1]


def level_of(own_key, extent, shards, least, high):
    level, own = 1.0, jax.random.fold_in(own_key, 6)
    for axis_at, parts in shards:
        heights = jnp.exp(jax.random.uniform(jax.random.fold_in(own, axis_at), (parts,), jnp.float32, least / len(shards), high / len(shards)))
        level = level * jnp.repeat(heights, extent[axis_at] // parts).reshape([-1 if axis == axis_at else 1 for axis in range(len(extent))])
    return level


def setup_inputs(seed: int = 0) -> dict:
    key_list = jax.random.split(jax.random.key(seed), 7)
    return {
        "volume": jnp.clip(jnp.exp(math.log(3.0) - 3.4011974 * jax.random.uniform(key_list[0], (NZ, NY, NU), jnp.float32) ** level_of(key_list[0], (NZ, NY, NU), ((0, 32), (1, 8)), -0.2, 0.2)), 0.1, 3.0),
        "measured": jnp.clip(2.0 * jax.random.uniform(key_list[1], (ANGLES, NR, NU), jnp.float32) ** level_of(key_list[1], (ANGLES, NR, NU), ((0, 8), (1, 32)), -0.2, 0.2), 0.0, 2.0).astype(jnp.bfloat16),
        "foot_start": draw_foot_start(jax.random.fold_in(key_list[6], 71), 0),
        "foot_len": draw_foot_len(jax.random.fold_in(key_list[6], 71), 0),
        "order": jax.random.permutation(key_list[4], ALL_ANG).astype(jnp.int32),
        "ray_table": jnp.clip(jnp.exp(jax.random.uniform(key_list[5], (ALL_ANG, NY), jnp.float32, math.log(0.001953125), math.log(0.0078125))), 0.001953125, 0.0078125),
    }


def hat_weights(starts, lengths, rows):
    first = starts[..., None, None]
    span_len = lengths[..., None, None]
    span = span_len / ZDEV
    centre = first + (jnp.arange(ZDEV, dtype=jnp.float32)[None, :] + 0.5) * span
    row_pos = rows[:, None]
    weight = jnp.maximum(0.0, 1.0 - jnp.abs(row_pos + 0.5 - centre) / span)
    inside = jnp.logical_and(row_pos >= first, row_pos < first + span_len)
    return jnp.where(inside, weight, 0.0)


def reference(volume, measured, foot_start, foot_len, order, ray_table):
    high = lax.Precision.HIGHEST
    picked = order[:ANGLES]
    onehot = (picked[:, None] == jnp.arange(ALL_ANG, dtype=jnp.int32)[None, :]).astype(jnp.float32)
    weights = jnp.dot(onehot, ray_table, precision=high)
    path = weights.sum(1)
    rows = jnp.arange(NR, dtype=jnp.float32)
    kernel = hat_weights(foot_start.T.astype(jnp.float32), foot_len.T.astype(jnp.float32), rows)
    kernel = kernel.transpose(0, 2, 1, 3).reshape(ANGLES, NR, NZ)
    summed = jnp.einsum('ay,zyx->azx', weights, volume, precision=high)
    project = jnp.einsum('arz,azx->arx', kernel, summed, precision=high)
    coverage = kernel.sum(-1)
    denom = jnp.maximum(path[:, None] * coverage, 0.25)
    residual = (measured.astype(jnp.float32) - project) / denom[:, :, None]
    back = jnp.einsum('arz,arx->azx', kernel, residual, precision=high)
    update = jnp.einsum('ay,azx->zyx', weights, back, precision=high)
    column = jnp.einsum('ay,az->zy', weights, kernel.sum(1), precision=high)
    updated = volume + update / column[:, :, None]
    return updated, residual
```

```python
import functools

import jax
import jax.numpy as jnp
from jax import lax
from jax.experimental import pallas as pl
from jax.experimental.pallas import tpu as pltpu
from jax.sharding import PartitionSpec as P

ZDEV = 8
ANGLES = 8
CHUNKS = 8
UPDATE_COLUMNS = 512
MESH = pl.DeviceIdType.MESH
F32 = jnp.float32
BF16 = jnp.bfloat16

SIB, ODD, UP2, DOWN2 = range(4)
BACK = (SIB, ODD, DOWN2, UP2)
RAY, PAIR, SLAB, BACKPROJ, PAIR2, GATHER, MESSAGES = 0, 3, 4, 8, 12, 13, 16


def order_of_steps(chunks):
    wire = {0: ("y", 11.2), 1: ("x", 5.6), 2: ("s", 8.4), 3: ("s", 8.4), 4: ("x", 5.6), 5: ("y", 11.2)}
    work = {0: (2.4, 0.0), 1: (0.5, 0.1), 2: (0.3, 0.1), 3: (1.6, 0.4), 4: (0.3, 0.1), 5: (0.3, 0.1), 6: (0.0, 0.1)}
    free = {"y": 0.0, "x": 0.0, "s": 0.0}
    ready = {(0, c): 1.5 + 1.2 * (c + 1) / chunks for c in range(chunks)}
    now, steps = 0.0, []
    while ready:
        waiting = [k for k in ready if ready[k] <= now]
        if waiting:
            step = max(waiting, key=lambda k: (k[0], -k[1]))
        else:
            step = min(ready, key=lambda k: (ready[k], -k[0]))
        now = max(now, ready.pop(step)) + work[step[0]][0] / chunks + work[step[0]][1]
        steps.append(step)
        if step[0] in wire:
            link, total = wire[step[0]]
            begin = max(free[link], now)
            free[link] = begin + total / chunks
            ready[(step[0] + 1, step[1])] = free[link] + 2.2
    return steps


def hat(row, first, length, k):
    span = length / ZDEV
    centre = first + (k + 0.5) * span
    weight = jnp.maximum(0.0, 1.0 - jnp.abs(row + 0.5 - centre) / span)
    return jnp.where((row >= first) & (row < first + length), weight, 0.0)


def high_part(value):
    return value.astype(BF16).astype(F32)


def iota(shape, dim):
    return lax.broadcasted_iota(jnp.int32, shape, dim)


def exchange_kernel(
    chunks, width,
    order_ref, start_ref, length_ref, table_ref, volume_hbm, measured_hbm,
    residual_hbm, gathered_hbm, back_weights_hbm,
    vol, meas, part, ray_in, pair_out, pair_in, sums, sums_in, out_rows, back_out, back_in,
    both_out, both_in, gathered, params, neighbour_params, weights, picked,
    project_weights, spread_weights, scale, back_weights,
    load_sem, store_sem, send_sem, recv_sem, psend_sem, precv_sem,
):
    slab = lax.axis_index("slab")
    ang = lax.axis_index("ang")
    n_slab = lax.axis_size("slab")
    y = lax.rem(ang, 4)
    xl = ang // 4
    core = lax.rem(slab, 2)
    other = 1 - xl
    pair_dev = (slab, other * 4 + y)
    sib_dev = (slab + 1 - 2 * core, ang)
    odd_dev = (lax.rem(slab + 2 * core - 1 + n_slab, n_slab), other * 4 + y)
    up_dev = (lax.rem(slab + 2, n_slab), other * 4 + y)
    down_dev = (lax.rem(slab + n_slab - 2, n_slab), other * 4 + y)
    slab_devs = (sib_dev, odd_dev, up_dev, down_dev)
    y_of = [None] + [lax.rem(y + d, 4) for d in (1, 2, 3)]
    y_devs = [None] + [(slab, xl * 4 + y_of[d]) for d in (1, 2, 3)]

    loads = [
        pltpu.make_async_copy(volume_hbm.at[:, pl.ds(c * width, width)], vol.at[c], load_sem.at[c])
        for c in range(chunks)
    ]
    for copy in loads:
        copy.start()
    load_measured = pltpu.make_async_copy(measured_hbm, meas, load_sem.at[chunks])
    load_measured.start()

    barrier = pltpu.get_barrier_semaphore()
    greeted = (*y_devs[1:], pair_dev, *slab_devs)
    for device in greeted:
        pl.semaphore_signal(barrier, inc=1, device_id=device, device_id_type=MESH)

    first_here = jnp.full((8, 128), start_ref[0, 0], jnp.int32).astype(F32)
    length_here = jnp.full((8, 128), length_ref[0, 0], jnp.int32).astype(F32)
    params[y, xl, 0] = first_here
    params[y, xl, 1] = length_here

    for m in range(ANGLES):
        angle = (m % 2) * 4 + m // 2
        picked[pl.ds(m, 1), :] = table_ref[pl.ds(order_ref[angle], 1), :]
    cells = picked.shape[1]
    share = cells // 8
    pick = (iota((cells, cells), 0) == ang * share + lax.rem(iota((cells, cells), 1), share)).astype(F32)
    mine = jnp.dot(picked[...], pick, precision=lax.Precision.HIGHEST, preferred_element_type=F32)
    blocks = jnp.broadcast_to(mine[:, None, :], (ANGLES, ZDEV, cells)).reshape(ANGLES * ZDEV, cells)
    own_slice = lax.rem(iota(blocks.shape, 0), ZDEV) == iota(blocks.shape, 1) // share
    blocks = jnp.where(own_slice, blocks, 0.0)
    weights[...] = blocks
    blocks_high = high_part(blocks)
    ray_weights = jnp.concatenate([blocks_high, blocks - blocks_high], axis=0).astype(BF16)

    pl.semaphore_wait(barrier, len(greeted))

    def remote(src, dst, sem, c, device, out_sem=None):
        return pltpu.make_async_remote_copy(
            src_ref=src, dst_ref=dst,
            send_sem=send_sem.at[c, sem if out_sem is None else out_sem],
            recv_sem=recv_sem.at[c, sem], device_id=device, device_id_type=MESH,
        )

    def param_copy(src, dst, k, device):
        return pltpu.make_async_remote_copy(
            src_ref=src, dst_ref=dst, send_sem=psend_sem.at[k], recv_sem=precv_sem.at[k],
            device_id=device, device_id_type=MESH,
        )

    own_params = params.at[y, xl]
    param_first = [
        param_copy(own_params, own_params, 0, pair_dev),
        param_copy(own_params, neighbour_params.at[SIB], 1, sib_dev),
    ]
    param_second = [
        param_copy(params.at[y, other], neighbour_params.at[ODD], 2, odd_dev),
        param_copy(params.at[y, other], neighbour_params.at[DOWN2], 3, up_dev),
        param_copy(params.at[y, other], neighbour_params.at[UP2], 4, down_dev),
    ] + [param_copy(params.at[y], params.at[y], 4 + d, y_devs[d]) for d in (1, 2, 3)]
    for copy in param_first:
        copy.start()

    ray = [[remote(part.at[c, y_of[d]], ray_in.at[c, d - 1], RAY + d - 1, c, y_devs[d]) for d in (1, 2, 3)] for c in range(chunks)]
    pair = [remote(pair_out.at[c], pair_in.at[c], PAIR, c, pair_dev) for c in range(chunks)]
    to_slab = [
        [
            remote(sums.at[c, xl if k == SIB else other], sums_in.at[c, BACK[k]], SLAB + BACK[k], c, slab_devs[k], SLAB + k)
            for k in range(4)
        ]
        for c in range(chunks)
    ]
    to_back = [
        [
            remote(back_out.at[c, 1 + k], back_in.at[c, BACK[k]], BACKPROJ + BACK[k], c, slab_devs[k], BACKPROJ + k)
            for k in range(4)
        ]
        for c in range(chunks)
    ]
    pair2 = [remote(both_out.at[c], both_in.at[c], PAIR2, c, pair_dev) for c in range(chunks)]
    gather = [[remote(gathered.at[c, y], gathered.at[c, y], GATHER + d - 1, c, y_devs[d]) for d in (1, 2, 3)] for c in range(chunks)]
    stores = []

    def wait_in(copies):
        for copy in copies:
            copy.wait_recv()

    def tables():
        wait_in(param_second)
        tiles = [params[y, xl]] + [neighbour_params[k] for k in range(4)]
        rows = first_here.shape[0] * 4
        lane = iota((rows, 128), 1)
        row = (slab * rows + iota((rows, 128), 0)).astype(F32)
        third = (lane >= 40).astype(jnp.int32) + (lane >= 80).astype(jnp.int32) + (lane >= 120).astype(jnp.int32)
        within = lane - 40 * third
        role = lax.shift_right_logical(within, 3)
        first = jnp.zeros((rows, 128), F32)
        length = jnp.full((rows, 128), 32.0, F32)
        for k in range(5):
            first = jnp.where(role == k, tiles[k][0, 0:1, :], first)
            length = jnp.where(role == k, tiles[k][1, 0:1, :], length)
        weight = hat(row, first, length, lax.bitwise_and(within, 7).astype(F32))
        high = high_part(weight)
        project_weights[...] = jnp.where(third < 2, high, jnp.where(third == 2, weight - high, 0.0)).astype(BF16)
        coverage = jnp.sum(jnp.where(third == 0, weight, 0.0), axis=1, keepdims=True)
        path = jnp.sum(table_ref[pl.ds(order_ref[ang], 1), :], axis=1, keepdims=True)
        scale[...] = jnp.broadcast_to(1.0 / jnp.maximum(path * coverage, 0.25), scale.shape)
        lane = iota((8, 128), 1)
        quarter = lax.shift_right_logical(lane, 5)
        row = (slab * rows + lax.bitwise_and(lane, 31)).astype(F32)
        k8 = iota((8, 128), 0).astype(F32)
        spread = []
        for k in range(5):
            weight = hat(row, tiles[k][0], tiles[k][1], k8)
            high = high_part(weight)
            spread.append(jnp.where(quarter < 2, high, jnp.where(quarter == 2, weight - high, 0.0)))
        spread.append(jnp.zeros((8, 128), F32))
        spread_weights[...] = jnp.concatenate(spread, axis=0).astype(BF16)

    def update_weights():
        lane = iota((8, 128), 1)
        base = (slab - 2) * 32
        k8 = iota((8, 128), 0).astype(F32)
        column = jnp.zeros((8, cells), F32)
        for m in range(ANGLES):
            tile_first, tile_length = params[m // 2, m % 2, 0], params[m // 2, m % 2, 1]
            near = hat((base + lane).astype(F32), tile_first, tile_length, k8)
            far = hat((base + 128 + lane).astype(F32), tile_first, tile_length, k8)
            slice_weight = jnp.sum(near + far, axis=1, keepdims=True)
            column = column + weights[m * 8 : m * 8 + 8, :] * slice_weight
        column = jnp.sum(column, axis=0, keepdims=True)
        ratio = weights[...] / column
        high = high_part(ratio)
        stack = jnp.concatenate([high, high, ratio - high, jnp.zeros_like(high)], axis=0)
        back_weights[...] = stack.T.astype(BF16)
        copy = pltpu.make_async_copy(back_weights, back_weights_hbm, store_sem.at[2 * chunks])
        copy.start()
        stores.append(copy)

    def ray_sums(c):
        loads[c].wait()
        value = vol[c]
        high = value.astype(BF16)
        low = (value - high.astype(F32)).astype(BF16)
        first = jnp.dot(ray_weights, high, preferred_element_type=F32)
        second = jnp.dot(ray_weights[: ANGLES * ZDEV], low, preferred_element_type=F32)
        total = first[: ANGLES * ZDEV] + first[ANGLES * ZDEV :] + second
        part[c] = total.reshape(part.shape[1:])
        for copy in ray[c]:
            copy.start()

    def ray_arrived(c):
        wait_in(ray[c])
        pair_out[c] = part[c, y] + ray_in[c, 0] + ray_in[c, 1] + ray_in[c, 2]
        pair[c].start()

    def pair_arrived(c):
        wait_in([pair[c]])
        sums[c] = pair_out[c] + pair_in[c]
        for copy in to_slab[c]:
            copy.start()

    def project(c):
        wait_in(to_slab[c])
        five = jnp.concatenate([sums[c, xl]] + [sums_in[c, k] for k in range(4)], axis=0)
        high = high_part(five)
        stack = jnp.concatenate([high, five - high, high, jnp.zeros((8, width), F32)], axis=0).astype(BF16)
        projected = jnp.dot(project_weights[...], stack, preferred_element_type=F32)
        here = (meas[:, c * width : (c + 1) * width].astype(F32) - projected) * scale[:, 0:1]
        out_rows[c] = here
        high = high_part(here)
        stack = jnp.concatenate([high, here - high, high, jnp.zeros_like(high)], axis=0).astype(BF16)
        spread = jnp.dot(spread_weights[...], stack, preferred_element_type=F32)
        back_out[c] = spread[:40].reshape(back_out.shape[1:])
        for copy in to_back[c]:
            copy.start()
        copy = pltpu.make_async_copy(out_rows.at[c], residual_hbm.at[:, pl.ds(c * width, width)], store_sem.at[c])
        copy.start()
        stores.append(copy)

    def back_arrived(c):
        wait_in(to_back[c])
        both_out[c, xl] = back_out[c, 0] + back_in[c, SIB]
        both_out[c, other] = back_in[c, ODD] + back_in[c, UP2] + back_in[c, DOWN2]
        pair2[c].start()

    def pair2_arrived(c):
        wait_in([pair2[c]])
        gathered[c, y] = both_out[c] + both_in[c]
        for copy in gather[c]:
            copy.start()

    def gather_arrived(c):
        wait_in(gather[c])
        copy = pltpu.make_async_copy(gathered.at[c], gathered_hbm.at[:, :, :, pl.ds(c * width, width)], store_sem.at[chunks + c])
        copy.start()
        stores.append(copy)

    stages = (ray_sums, ray_arrived, pair_arrived, project, back_arrived, pair2_arrived, gather_arrived)
    forwarded = False
    done_tables = False
    done_update = False
    for stage, c in order_of_steps(chunks):
        if stage == 1 and not forwarded:
            wait_in(param_first)
            for copy in param_second:
                copy.start()
            forwarded = True
        if stage == 3 and not done_tables:
            load_measured.wait()
            tables()
            done_tables = True
        if stage == 4 and not done_update:
            update_weights()
            done_update = True
        stages[stage](c)

    for copy in param_first + param_second:
        copy.wait_send()
    for group in ray + to_slab + to_back + gather:
        for copy in group:
            copy.wait_send()
    for copy in pair + pair2:
        copy.wait_send()
    for copy in stores:
        copy.wait()


def update_kernel(weights_ref, volume_ref, gathered_ref, out_ref):
    value = gathered_ref[...]
    high = high_part(value)
    stack = jnp.concatenate([high, value - high, high, jnp.zeros_like(high)], axis=0).astype(BF16)
    out_ref[...] = volume_ref[...] + jnp.dot(weights_ref[...], stack, preferred_element_type=F32)


def body(volume, measured, foot_start, foot_len, order, ray_table):
    slices, share, columns = volume.shape
    cells = slices * share
    rows = measured.shape[1]
    flat = volume.reshape(cells, columns)
    chunks = CHUNKS
    width = columns // chunks
    vmem = pltpu.VMEM
    smem = pl.BlockSpec(memory_space=pltpu.SMEM)
    hbm = pl.BlockSpec(memory_space=pl.ANY)
    residual, gathered, back_weights = pl.pallas_call(
        functools.partial(exchange_kernel, chunks, width),
        out_shape=(
            jax.ShapeDtypeStruct((rows, columns), F32),
            jax.ShapeDtypeStruct((4, 2, ZDEV, columns), F32),
            jax.ShapeDtypeStruct((cells, 4 * ANGLES * ZDEV), BF16),
        ),
        in_specs=[smem, smem, smem, pl.BlockSpec(memory_space=pltpu.VMEM), hbm, hbm],
        out_specs=(hbm, hbm, hbm),
        scratch_shapes=[
            vmem((chunks, cells, width), F32),
            vmem((rows, columns), BF16),
            vmem((chunks, 4, 2, ZDEV, width), F32),
            vmem((chunks, 3, 2, ZDEV, width), F32),
            vmem((chunks, 2, ZDEV, width), F32),
            vmem((chunks, 2, ZDEV, width), F32),
            vmem((chunks, 2, ZDEV, width), F32),
            vmem((chunks, 4, ZDEV, width), F32),
            vmem((chunks, rows, width), F32),
            vmem((chunks, 5, ZDEV, width), F32),
            vmem((chunks, 4, ZDEV, width), F32),
            vmem((chunks, 2, ZDEV, width), F32),
            vmem((chunks, 2, ZDEV, width), F32),
            vmem((chunks, 4, 2, ZDEV, width), F32),
            vmem((4, 2, 2, 8, 128), F32),
            vmem((4, 2, 8, 128), F32),
            vmem((ANGLES * ZDEV, cells), F32),
            vmem((ANGLES, ray_table.shape[1]), F32),
            vmem((rows, 128), BF16),
            vmem((48, 128), BF16),
            vmem((rows, 128), F32),
            vmem((cells, 4 * ANGLES * ZDEV), BF16),
            pltpu.SemaphoreType.DMA((chunks + 1,)),
            pltpu.SemaphoreType.DMA((2 * chunks + 1,)),
            pltpu.SemaphoreType.DMA((chunks, MESSAGES)),
            pltpu.SemaphoreType.DMA((chunks, MESSAGES)),
            pltpu.SemaphoreType.DMA((8,)),
            pltpu.SemaphoreType.DMA((8,)),
        ],
        compiler_params=pltpu.CompilerParams(
            collective_id=0, has_side_effects=True, vmem_limit_bytes=40 * 1024 * 1024
        ),
        name="exchange",
    )(order, foot_start, foot_len, ray_table, flat, measured.reshape(rows, columns))
    block = UPDATE_COLUMNS
    updated = pl.pallas_call(
        update_kernel,
        out_shape=jax.ShapeDtypeStruct((cells, columns), F32),
        grid=(columns // block,),
        in_specs=[
            pl.BlockSpec((cells, 4 * ANGLES * ZDEV), lambda i: (0, 0)),
            pl.BlockSpec((cells, block), lambda i: (0, i)),
            pl.BlockSpec((ANGLES * ZDEV, block), lambda i: (0, i)),
        ],
        out_specs=pl.BlockSpec((cells, block), lambda i: (0, i)),
        name="update",
    )(back_weights, flat, gathered.reshape(ANGLES * ZDEV, columns))
    return (updated.reshape(slices, share, columns), residual.reshape(measured.shape))


def solution(mesh):
    return jax.shard_map(
        body,
        mesh=mesh,
        in_specs=(
            P("slab", "ang", None),
            P("ang", "slab", None),
            P("slab", "ang"),
            P("slab", "ang"),
            P(),
            P(),
        ),
        out_specs=(P("slab", "ang", None), P("ang", "slab", None)),
        check_vma=False,
    )
```

```python
import functools

import jax
import jax.numpy as jnp
from jax import lax
from jax.experimental import pallas as pl
from jax.experimental.pallas import tpu as pltpu
from jax.sharding import PartitionSpec as P

ZDEV = 8
ANGLES = 8
CHUNKS = 8
MESH = pl.DeviceIdType.MESH
F32 = jnp.float32
BF16 = jnp.bfloat16

SIB, ODD, UP2, DOWN2 = range(4)
BACK = (SIB, ODD, DOWN2, UP2)
RAY, PAIR, SLAB, BACKPROJ, PAIR2, GATHER, MESSAGES = 0, 3, 4, 8, 12, 13, 16


def order_of_steps(chunks):
    wire = {0: ("y", 11.2), 1: ("x", 5.6), 2: ("s", 8.4), 3: ("s", 8.4), 4: ("x", 5.6), 5: ("y", 11.2)}
    work = {0: (2.4, 0.0), 1: (0.5, 0.1), 2: (0.3, 0.1), 3: (1.6, 0.4), 4: (0.3, 0.1), 5: (0.3, 0.1), 6: (0.0, 0.1)}
    free = {"y": 0.0, "x": 0.0, "s": 0.0}
    ready = {(0, c): 1.5 + 1.2 * (c + 1) / chunks for c in range(chunks)}
    now, steps = 0.0, []
    while ready:
        waiting = [k for k in ready if ready[k] <= now]
        if waiting:
            step = max(waiting, key=lambda k: (k[0], -k[1]))
        else:
            step = min(ready, key=lambda k: (ready[k], -k[0]))
        now = max(now, ready.pop(step)) + work[step[0]][0] / chunks + work[step[0]][1]
        steps.append(step)
        if step[0] in wire:
            link, total = wire[step[0]]
            begin = max(free[link], now)
            free[link] = begin + total / chunks
            ready[(step[0] + 1, step[1])] = free[link] + 2.2
    return steps


def hat(row, first, length, k):
    span = length / ZDEV
    centre = first + (k + 0.5) * span
    weight = jnp.maximum(0.0, 1.0 - jnp.abs(row + 0.5 - centre) / span)
    return jnp.where((row >= first) & (row < first + length), weight, 0.0)


def high_part(value):
    return value.astype(BF16).astype(F32)


def iota(shape, dim):
    return lax.broadcasted_iota(jnp.int32, shape, dim)


def exchange_kernel(
    chunks, width,
    start_ref, length_ref, order_hbm, table_hbm, volume_hbm, measured_hbm,
    updated_ref, residual_ref,
    vol, meas, order_ref, table_ref, part, ray_in, pair_out, pair_in, sums, sums_in, back_out, back_in,
    both_out, both_in, gathered, params, neighbour_params, weights, picked,
    project_weights, spread_weights, scale, back_weights,
    load_sem, send_sem, recv_sem, psend_sem, precv_sem,
):
    slab = lax.axis_index("slab")
    ang = lax.axis_index("ang")
    n_slab = lax.axis_size("slab")
    y = lax.rem(ang, 4)
    xl = ang // 4
    core = lax.rem(slab, 2)
    other = 1 - xl
    pair_dev = (slab, other * 4 + y)
    sib_dev = (slab + 1 - 2 * core, ang)
    odd_dev = (lax.rem(slab + 2 * core - 1 + n_slab, n_slab), other * 4 + y)
    up_dev = (lax.rem(slab + 2, n_slab), other * 4 + y)
    down_dev = (lax.rem(slab + n_slab - 2, n_slab), other * 4 + y)
    slab_devs = (sib_dev, odd_dev, up_dev, down_dev)
    y_of = [None] + [lax.rem(y + d, 4) for d in (1, 2, 3)]
    y_devs = [None] + [(slab, xl * 4 + y_of[d]) for d in (1, 2, 3)]

    load_order = pltpu.make_async_copy(order_hbm, order_ref, load_sem.at[chunks + 2])
    load_order.start()
    load_table = pltpu.make_async_copy(table_hbm, table_ref, load_sem.at[chunks + 1])
    load_table.start()
    loads = [
        pltpu.make_async_copy(volume_hbm.at[:, pl.ds(c * width, width)], vol.at[c], load_sem.at[c])
        for c in range(chunks)
    ]
    for copy in loads:
        copy.start()
    load_measured = pltpu.make_async_copy(measured_hbm, meas, load_sem.at[chunks])
    load_measured.start()

    barrier = pltpu.get_barrier_semaphore()
    greeted = (*y_devs[1:], pair_dev, *slab_devs)
    for device in greeted:
        pl.semaphore_signal(barrier, inc=1, device_id=device, device_id_type=MESH)

    first_here = jnp.full((8, 128), start_ref[0, 0], jnp.int32).astype(F32)
    length_here = jnp.full((8, 128), length_ref[0, 0], jnp.int32).astype(F32)
    params[y, xl, 0] = first_here
    params[y, xl, 1] = length_here

    load_order.wait()
    load_table.wait()
    for m in range(ANGLES):
        angle = (m % 2) * 4 + m // 2
        picked[pl.ds(m, 1), :] = table_ref[pl.ds(order_ref[angle], 1), :]
    cells = picked.shape[1]
    share = cells // 8
    pick = (iota((cells, cells), 0) == ang * share + lax.rem(iota((cells, cells), 1), share)).astype(F32)
    mine = jnp.dot(picked[...], pick, precision=lax.Precision.HIGHEST, preferred_element_type=F32)
    blocks = jnp.broadcast_to(mine[:, None, :], (ANGLES, ZDEV, cells)).reshape(ANGLES * ZDEV, cells)
    own_slice = lax.rem(iota(blocks.shape, 0), ZDEV) == iota(blocks.shape, 1) // share
    blocks = jnp.where(own_slice, blocks, 0.0)
    weights[...] = blocks
    blocks_high = high_part(blocks)
    ray_weights = jnp.concatenate([blocks_high, blocks - blocks_high], axis=0).astype(BF16)

    pl.semaphore_wait(barrier, len(greeted))

    def remote(src, dst, sem, c, device, out_sem=None):
        return pltpu.make_async_remote_copy(
            src_ref=src, dst_ref=dst,
            send_sem=send_sem.at[c, sem if out_sem is None else out_sem],
            recv_sem=recv_sem.at[c, sem], device_id=device, device_id_type=MESH,
        )

    def param_copy(src, dst, k, device):
        return pltpu.make_async_remote_copy(
            src_ref=src, dst_ref=dst, send_sem=psend_sem.at[k], recv_sem=precv_sem.at[k],
            device_id=device, device_id_type=MESH,
        )

    own_params = params.at[y, xl]
    param_first = [
        param_copy(own_params, own_params, 0, pair_dev),
        param_copy(own_params, neighbour_params.at[SIB], 1, sib_dev),
    ]
    param_second = [
        param_copy(params.at[y, other], neighbour_params.at[ODD], 2, odd_dev),
        param_copy(params.at[y, other], neighbour_params.at[DOWN2], 3, up_dev),
        param_copy(params.at[y, other], neighbour_params.at[UP2], 4, down_dev),
    ] + [param_copy(params.at[y], params.at[y], 4 + d, y_devs[d]) for d in (1, 2, 3)]
    for copy in param_first:
        copy.start()

    ray = [[remote(part.at[c, y_of[d]], ray_in.at[c, d - 1], RAY + d - 1, c, y_devs[d]) for d in (1, 2, 3)] for c in range(chunks)]
    pair = [remote(pair_out.at[c], pair_in.at[c], PAIR, c, pair_dev) for c in range(chunks)]
    to_slab = [
        [
            remote(sums.at[c, xl if k == SIB else other], sums_in.at[c, BACK[k]], SLAB + BACK[k], c, slab_devs[k], SLAB + k)
            for k in range(4)
        ]
        for c in range(chunks)
    ]
    to_back = [
        [
            remote(back_out.at[c, 1 + k], back_in.at[c, BACK[k]], BACKPROJ + BACK[k], c, slab_devs[k], BACKPROJ + k)
            for k in range(4)
        ]
        for c in range(chunks)
    ]
    pair2 = [remote(both_out.at[c], both_in.at[c], PAIR2, c, pair_dev) for c in range(chunks)]
    gather = [[remote(gathered.at[c, y], gathered.at[c, y], GATHER + d - 1, c, y_devs[d]) for d in (1, 2, 3)] for c in range(chunks)]
    def wait_in(copies):
        for copy in copies:
            copy.wait_recv()

    def tables():
        wait_in(param_second)
        tiles = [params[y, xl]] + [neighbour_params[k] for k in range(4)]
        rows = first_here.shape[0] * 4
        lane = iota((rows, 128), 1)
        row = (slab * rows + iota((rows, 128), 0)).astype(F32)
        third = (lane >= 40).astype(jnp.int32) + (lane >= 80).astype(jnp.int32) + (lane >= 120).astype(jnp.int32)
        within = lane - 40 * third
        role = lax.shift_right_logical(within, 3)
        first = jnp.zeros((rows, 128), F32)
        length = jnp.full((rows, 128), 32.0, F32)
        for k in range(5):
            first = jnp.where(role == k, tiles[k][0, 0:1, :], first)
            length = jnp.where(role == k, tiles[k][1, 0:1, :], length)
        weight = hat(row, first, length, lax.bitwise_and(within, 7).astype(F32))
        high = high_part(weight)
        project_weights[...] = jnp.where(third < 2, high, jnp.where(third == 2, weight - high, 0.0)).astype(BF16)
        coverage = jnp.sum(jnp.where(third == 0, weight, 0.0), axis=1, keepdims=True)
        path = jnp.sum(table_ref[pl.ds(order_ref[ang], 1), :], axis=1, keepdims=True)
        scale[...] = jnp.broadcast_to(1.0 / jnp.maximum(path * coverage, 0.25), scale.shape)
        lane = iota((8, 128), 1)
        quarter = lax.shift_right_logical(lane, 5)
        row = (slab * rows + lax.bitwise_and(lane, 31)).astype(F32)
        k8 = iota((8, 128), 0).astype(F32)
        spread = []
        for k in range(5):
            weight = hat(row, tiles[k][0], tiles[k][1], k8)
            high = high_part(weight)
            spread.append(jnp.where(quarter < 2, high, jnp.where(quarter == 2, weight - high, 0.0)))
        spread.append(jnp.zeros((8, 128), F32))
        spread_weights[...] = jnp.concatenate(spread, axis=0).astype(BF16)

    def update_weights():
        lane = iota((8, 128), 1)
        base = (slab - 2) * 32
        k8 = iota((8, 128), 0).astype(F32)
        column = jnp.zeros((8, cells), F32)
        for m in range(ANGLES):
            tile_first, tile_length = params[m // 2, m % 2, 0], params[m // 2, m % 2, 1]
            near = hat((base + lane).astype(F32), tile_first, tile_length, k8)
            far = hat((base + 128 + lane).astype(F32), tile_first, tile_length, k8)
            slice_weight = jnp.sum(near + far, axis=1, keepdims=True)
            column = column + weights[m * 8 : m * 8 + 8, :] * slice_weight
        column = jnp.sum(column, axis=0, keepdims=True)
        ratio = weights[...] / column
        high = high_part(ratio)
        stack = jnp.concatenate([high, high, ratio - high, jnp.zeros_like(high)], axis=0)
        back_weights[...] = stack.T.astype(BF16)

    def ray_sums(c):
        loads[c].wait()
        value = vol[c]
        high = value.astype(BF16)
        low = (value - high.astype(F32)).astype(BF16)
        first = jnp.dot(ray_weights, high, preferred_element_type=F32)
        second = jnp.dot(ray_weights[: ANGLES * ZDEV], low, preferred_element_type=F32)
        total = first[: ANGLES * ZDEV] + first[ANGLES * ZDEV :] + second
        part[c] = total.reshape(part.shape[1:])
        for copy in ray[c]:
            copy.start()

    def ray_arrived(c):
        wait_in(ray[c])
        pair_out[c] = part[c, y] + ray_in[c, 0] + ray_in[c, 1] + ray_in[c, 2]
        pair[c].start()

    def pair_arrived(c):
        wait_in([pair[c]])
        sums[c] = pair_out[c] + pair_in[c]
        for copy in to_slab[c]:
            copy.start()

    def project(c):
        wait_in(to_slab[c])
        five = jnp.concatenate([sums[c, xl]] + [sums_in[c, k] for k in range(4)], axis=0)
        high = high_part(five)
        stack = jnp.concatenate([high, five - high, high, jnp.zeros((8, width), F32)], axis=0).astype(BF16)
        projected = jnp.dot(project_weights[...], stack, preferred_element_type=F32)
        here = (meas[:, c * width : (c + 1) * width].astype(F32) - projected) * scale[:, 0:1]
        residual_ref[:, c * width : (c + 1) * width] = here
        high = high_part(here)
        stack = jnp.concatenate([high, here - high, high, jnp.zeros_like(high)], axis=0).astype(BF16)
        spread = jnp.dot(spread_weights[...], stack, preferred_element_type=F32)
        back_out[c] = spread[:40].reshape(back_out.shape[1:])
        for copy in to_back[c]:
            copy.start()

    def back_arrived(c):
        wait_in(to_back[c])
        both_out[c, xl] = back_out[c, 0] + back_in[c, SIB]
        both_out[c, other] = back_in[c, ODD] + back_in[c, UP2] + back_in[c, DOWN2]
        pair2[c].start()

    def pair2_arrived(c):
        wait_in([pair2[c]])
        gathered[c, y] = both_out[c] + both_in[c]
        for copy in gather[c]:
            copy.start()

    def gather_arrived(c):
        wait_in(gather[c])
        value = gathered[c].reshape(ANGLES * ZDEV, width)
        high = high_part(value)
        stack = jnp.concatenate([high, value - high, high, jnp.zeros_like(high)], axis=0).astype(BF16)
        update = jnp.dot(back_weights[...], stack, preferred_element_type=F32)
        updated_ref[:, c * width : (c + 1) * width] = vol[c] + update

    stages = (ray_sums, ray_arrived, pair_arrived, project, back_arrived, pair2_arrived, gather_arrived)
    forwarded = False
    done_tables = False
    done_update = False
    for stage, c in order_of_steps(chunks):
        if stage == 1 and not forwarded:
            wait_in(param_first)
            for copy in param_second:
                copy.start()
            forwarded = True
        if stage == 3 and not done_tables:
            load_measured.wait()
            tables()
            done_tables = True
        if stage == 4 and not done_update:
            update_weights()
            done_update = True
        stages[stage](c)

    for copy in param_first + param_second:
        copy.wait_send()
    for group in ray + to_slab + to_back + gather:
        for copy in group:
            copy.wait_send()
    for copy in pair + pair2:
        copy.wait_send()


def body(volume, measured, foot_start, foot_len, order, ray_table):
    slices, share, columns = volume.shape
    cells = slices * share
    rows = measured.shape[1]
    flat = volume.reshape(cells, columns)
    chunks = CHUNKS
    width = columns // chunks
    vmem = pltpu.VMEM
    smem = pl.BlockSpec(memory_space=pltpu.SMEM)
    hbm = pl.BlockSpec(memory_space=pltpu.HBM)
    updated, residual = pl.pallas_call(
        functools.partial(exchange_kernel, chunks, width),
        out_shape=(
            jax.ShapeDtypeStruct((cells, columns), F32),
            jax.ShapeDtypeStruct((rows, columns), F32),
        ),
        in_specs=[smem, smem, hbm, hbm, hbm, hbm],
        out_specs=(pl.BlockSpec(memory_space=pltpu.VMEM),) * 2,
        scratch_shapes=[
            vmem((chunks, cells, width), F32),
            vmem((rows, columns), BF16),
            pltpu.SMEM(order.shape, jnp.int32),
            vmem(ray_table.shape, F32),
            vmem((chunks, 4, 2, ZDEV, width), F32),
            vmem((chunks, 3, 2, ZDEV, width), F32),
            vmem((chunks, 2, ZDEV, width), F32),
            vmem((chunks, 2, ZDEV, width), F32),
            vmem((chunks, 2, ZDEV, width), F32),
            vmem((chunks, 4, ZDEV, width), F32),
            vmem((chunks, 5, ZDEV, width), F32),
            vmem((chunks, 4, ZDEV, width), F32),
            vmem((chunks, 2, ZDEV, width), F32),
            vmem((chunks, 2, ZDEV, width), F32),
            vmem((chunks, 4, 2, ZDEV, width), F32),
            vmem((4, 2, 2, 8, 128), F32),
            vmem((4, 2, 8, 128), F32),
            vmem((ANGLES * ZDEV, cells), F32),
            vmem((ANGLES, ray_table.shape[1]), F32),
            vmem((rows, 128), BF16),
            vmem((48, 128), BF16),
            vmem((rows, 128), F32),
            vmem((cells, 4 * ANGLES * ZDEV), BF16),
            pltpu.SemaphoreType.DMA((chunks + 3,)),
            pltpu.SemaphoreType.DMA((chunks, MESSAGES)),
            pltpu.SemaphoreType.DMA((chunks, MESSAGES)),
            pltpu.SemaphoreType.DMA((8,)),
            pltpu.SemaphoreType.DMA((8,)),
        ],
        compiler_params=pltpu.CompilerParams(
            collective_id=0, has_side_effects=True, vmem_limit_bytes=40 * 1024 * 1024
        ),
        name="exchange",
    )(
        foot_start, foot_len, *(
            pltpu.with_memory_space_constraint(a, pltpu.HBM)
            for a in (order, ray_table, flat, measured.reshape(rows, columns))
        )
    )
    return (updated.reshape(slices, share, columns), residual.reshape(measured.shape))


def solution(mesh):
    return jax.shard_map(
        body,
        mesh=mesh,
        in_specs=(
            P("slab", "ang", None),
            P("ang", "slab", None),
            P("slab", "ang"),
            P("slab", "ang"),
            P(),
            P(),
        ),
        out_specs=(P("slab", "ang", None), P("ang", "slab", None)),
        check_vma=False,
    )
```

```python
import functools

import jax
import jax.numpy as jnp
from jax import lax
from jax.experimental import pallas as pl
from jax.experimental.pallas import tpu as pltpu
from jax.sharding import PartitionSpec as P

ZDEV = 8
ANGLES = 8
CHUNKS = 8
LAG = 2.5
MESH = pl.DeviceIdType.MESH
F32 = jnp.float32
BF16 = jnp.bfloat16

SIB, ODD, UP2, DOWN2 = range(4)
BACK = (SIB, ODD, DOWN2, UP2)
FAR_FIRST = (UP2, DOWN2, ODD, SIB)
RAY, PAIR, SLAB, BACKPROJ, PAIR2, GATHER, EXCHANGES = range(7)
SENT_ROWS = (48, 16, 32, 32, 16, 48)


def order_of_steps(chunks):
    steps = [(k, c) for k in range(7) for c in range(chunks)]
    return sorted(steps, key=lambda step: (step[1] + LAG * step[0], -step[0]))


def hat(row, first, length, k):
    span = length / ZDEV
    centre = first + (k + 0.5) * span
    weight = jnp.maximum(0.0, 1.0 - jnp.abs(row + 0.5 - centre) / span)
    return jnp.where((row >= first) & (row < first + length), weight, 0.0)


def high_part(value):
    return value.astype(BF16).astype(F32)


def iota(shape, dim):
    return lax.broadcasted_iota(jnp.int32, shape, dim)


def exchange_kernel(
    chunks, width,
    start_ref, length_ref, order_hbm, table_hbm, volume_hbm, measured_hbm,
    updated_ref, residual_ref,
    vol, meas, order_ref, table_ref, part, ray_in, pair_out, pair_in, sums, sums_in, back_out, back_in,
    both_out, both_in, gathered, params, neighbour_params, weights, picked,
    project_weights, spread_weights, scale, back_weights,
    load_sem, send_sem, recv_sem, psend_sem, precv_sem,
):
    slab = lax.axis_index("slab")
    ang = lax.axis_index("ang")
    n_slab = lax.axis_size("slab")
    y = lax.rem(ang, 4)
    xl = ang // 4
    core = lax.rem(slab, 2)
    other = 1 - xl
    pair_dev = (slab, other * 4 + y)
    sib_dev = (slab + 1 - 2 * core, ang)
    odd_dev = (lax.rem(slab + 2 * core - 1 + n_slab, n_slab), other * 4 + y)
    up_dev = (lax.rem(slab + 2, n_slab), other * 4 + y)
    down_dev = (lax.rem(slab + n_slab - 2, n_slab), other * 4 + y)
    slab_devs = (sib_dev, odd_dev, up_dev, down_dev)
    y_of = [None] + [lax.rem(y + d, 4) for d in (1, 2, 3)]
    y_devs = [None] + [(slab, xl * 4 + y_of[d]) for d in (1, 2, 3)]

    load_order = pltpu.make_async_copy(order_hbm, order_ref, load_sem.at[chunks + 2])
    load_order.start()
    load_table = pltpu.make_async_copy(table_hbm, table_ref, load_sem.at[chunks + 1])
    load_table.start()
    loads = [
        pltpu.make_async_copy(volume_hbm.at[:, pl.ds(c * width, width)], vol.at[c], load_sem.at[c])
        for c in range(chunks)
    ]
    for copy in loads:
        copy.start()
    load_measured = pltpu.make_async_copy(measured_hbm, meas, load_sem.at[chunks])
    load_measured.start()

    barrier = pltpu.get_barrier_semaphore()
    greeted = (*y_devs[1:], pair_dev, *slab_devs)
    for device in greeted:
        pl.semaphore_signal(barrier, inc=1, device_id=device, device_id_type=MESH)

    first_here = jnp.full((8, 128), start_ref[0, 0], jnp.int32).astype(F32)
    length_here = jnp.full((8, 128), length_ref[0, 0], jnp.int32).astype(F32)
    params[y, xl, 0] = first_here
    params[y, xl, 1] = length_here

    load_order.wait()
    load_table.wait()
    for m in range(ANGLES):
        angle = (m % 2) * 4 + m // 2
        picked[pl.ds(m, 1), :] = table_ref[pl.ds(order_ref[angle], 1), :]
    cells = picked.shape[1]
    share = cells // 8
    pick = (iota((cells, cells), 0) == ang * share + lax.rem(iota((cells, cells), 1), share)).astype(F32)
    mine = jnp.dot(picked[...], pick, precision=lax.Precision.HIGHEST, preferred_element_type=F32)
    blocks = jnp.broadcast_to(mine[:, None, :], (ANGLES, ZDEV, cells)).reshape(ANGLES * ZDEV, cells)
    own_slice = lax.rem(iota(blocks.shape, 0), ZDEV) == iota(blocks.shape, 1) // share
    blocks = jnp.where(own_slice, blocks, 0.0)
    weights[...] = blocks
    blocks_high = high_part(blocks)
    ray_weights = jnp.concatenate([blocks_high, blocks - blocks_high], axis=0).astype(BF16)

    pl.semaphore_wait(barrier, len(greeted))

    def remote(src, dst, exchange, c, device):
        return pltpu.make_async_remote_copy(
            src_ref=src, dst_ref=dst, send_sem=send_sem.at[exchange], recv_sem=recv_sem.at[c, exchange],
            device_id=device, device_id_type=MESH,
        )

    def param_copy(src, dst, k, device):
        return pltpu.make_async_remote_copy(
            src_ref=src, dst_ref=dst, send_sem=psend_sem.at[k], recv_sem=precv_sem.at[k],
            device_id=device, device_id_type=MESH,
        )

    own_params = params.at[y, xl]
    param_first = [
        param_copy(own_params, own_params, 0, pair_dev),
        param_copy(own_params, neighbour_params.at[SIB], 1, sib_dev),
    ]
    param_second = [
        param_copy(params.at[y, other], neighbour_params.at[ODD], 2, odd_dev),
        param_copy(params.at[y, other], neighbour_params.at[DOWN2], 3, up_dev),
        param_copy(params.at[y, other], neighbour_params.at[UP2], 4, down_dev),
    ] + [param_copy(params.at[y], params.at[y], 4 + d, y_devs[d]) for d in (1, 2, 3)]
    for copy in param_first:
        copy.start()

    ray = [[remote(part.at[c, y_of[d]], ray_in.at[c, d - 1], RAY, c, y_devs[d]) for d in (1, 2, 3)] for c in range(chunks)]
    pair = [remote(pair_out.at[c], pair_in.at[c], PAIR, c, pair_dev) for c in range(chunks)]
    to_slab = [
        [remote(sums.at[c, xl if k == SIB else other], sums_in.at[c, BACK[k]], SLAB, c, slab_devs[k]) for k in FAR_FIRST]
        for c in range(chunks)
    ]
    to_back = [
        [remote(back_out.at[c, 1 + k], back_in.at[c, BACK[k]], BACKPROJ, c, slab_devs[k]) for k in FAR_FIRST]
        for c in range(chunks)
    ]
    pair2 = [remote(both_out.at[c], both_in.at[c], PAIR2, c, pair_dev) for c in range(chunks)]
    gather = [[remote(gathered.at[c, y], gathered.at[c, y], GATHER, c, y_devs[d]) for d in (1, 2, 3)] for c in range(chunks)]
    landing = (ray_in, pair_in, sums_in, back_in, both_in, gathered.at[:, pl.ds(0, 3)])

    def wait_in(copies):
        for copy in copies:
            copy.wait_recv()

    def wait_exchange(exchange, c):
        whole = landing[exchange].at[c]
        remote(whole, whole, exchange, c, pair_dev).wait_recv()

    def tables():
        wait_in(param_second)
        tiles = [params[y, xl]] + [neighbour_params[k] for k in range(4)]
        rows = first_here.shape[0] * 4
        lane = iota((rows, 128), 1)
        row = (slab * rows + iota((rows, 128), 0)).astype(F32)
        third = (lane >= 40).astype(jnp.int32) + (lane >= 80).astype(jnp.int32) + (lane >= 120).astype(jnp.int32)
        within = lane - 40 * third
        role = lax.shift_right_logical(within, 3)
        first = jnp.zeros((rows, 128), F32)
        length = jnp.full((rows, 128), 32.0, F32)
        for k in range(5):
            first = jnp.where(role == k, tiles[k][0, 0:1, :], first)
            length = jnp.where(role == k, tiles[k][1, 0:1, :], length)
        weight = hat(row, first, length, lax.bitwise_and(within, 7).astype(F32))
        high = high_part(weight)
        project_weights[...] = jnp.where(third < 2, high, jnp.where(third == 2, weight - high, 0.0)).astype(BF16)
        coverage = jnp.sum(jnp.where(third == 0, weight, 0.0), axis=1, keepdims=True)
        path = jnp.sum(table_ref[pl.ds(order_ref[ang], 1), :], axis=1, keepdims=True)
        scale[...] = jnp.broadcast_to(1.0 / jnp.maximum(path * coverage, 0.25), scale.shape)
        lane = iota((8, 128), 1)
        quarter = lax.shift_right_logical(lane, 5)
        row = (slab * rows + lax.bitwise_and(lane, 31)).astype(F32)
        k8 = iota((8, 128), 0).astype(F32)
        spread = []
        for k in range(5):
            weight = hat(row, tiles[k][0], tiles[k][1], k8)
            high = high_part(weight)
            spread.append(jnp.where(quarter < 2, high, jnp.where(quarter == 2, weight - high, 0.0)))
        spread.append(jnp.zeros((8, 128), F32))
        spread_weights[...] = jnp.concatenate(spread, axis=0).astype(BF16)

    def update_weights():
        lane = iota((8, 128), 1)
        base = (slab - 2) * 32
        k8 = iota((8, 128), 0).astype(F32)
        column = jnp.zeros((8, cells), F32)
        for m in range(ANGLES):
            tile_first, tile_length = params[m // 2, m % 2, 0], params[m // 2, m % 2, 1]
            near = hat((base + lane).astype(F32), tile_first, tile_length, k8)
            far = hat((base + 128 + lane).astype(F32), tile_first, tile_length, k8)
            slice_weight = jnp.sum(near + far, axis=1, keepdims=True)
            column = column + weights[m * 8 : m * 8 + 8, :] * slice_weight
        column = jnp.sum(column, axis=0, keepdims=True)
        ratio = weights[...] / column
        high = high_part(ratio)
        stack = jnp.concatenate([high, high, ratio - high, jnp.zeros_like(high)], axis=0)
        back_weights[...] = stack.T.astype(BF16)

    def ray_sums(c):
        loads[c].wait()
        value = vol[c]
        high = value.astype(BF16)
        low = (value - high.astype(F32)).astype(BF16)
        first = jnp.dot(ray_weights, high, preferred_element_type=F32)
        second = jnp.dot(ray_weights[: ANGLES * ZDEV], low, preferred_element_type=F32)
        total = first[: ANGLES * ZDEV] + first[ANGLES * ZDEV :] + second
        part[c] = total.reshape(part.shape[1:])
        for copy in ray[c]:
            copy.start()

    def ray_arrived(c):
        wait_exchange(RAY, c)
        pair_out[c] = part[c, y] + ray_in[c, 0] + ray_in[c, 1] + ray_in[c, 2]
        pair[c].start()

    def pair_arrived(c):
        wait_exchange(PAIR, c)
        sums[c] = pair_out[c] + pair_in[c]
        for copy in to_slab[c]:
            copy.start()

    def project(c):
        wait_exchange(SLAB, c)
        five = jnp.concatenate([sums[c, xl]] + [sums_in[c, k] for k in range(4)], axis=0)
        high = high_part(five)
        stack = jnp.concatenate([high, five - high, high, jnp.zeros((8, width), F32)], axis=0).astype(BF16)
        projected = jnp.dot(project_weights[...], stack, preferred_element_type=F32)
        here = (meas[:, c * width : (c + 1) * width].astype(F32) - projected) * scale[:, 0:1]
        residual_ref[:, c * width : (c + 1) * width] = here
        high = high_part(here)
        stack = jnp.concatenate([high, here - high, high, jnp.zeros_like(high)], axis=0).astype(BF16)
        spread = jnp.dot(spread_weights[...], stack, preferred_element_type=F32)
        back_out[c] = spread[:40].reshape(back_out.shape[1:])
        for copy in to_back[c]:
            copy.start()

    def back_arrived(c):
        wait_exchange(BACKPROJ, c)
        both_out[c, xl] = back_out[c, 0] + back_in[c, SIB]
        both_out[c, other] = back_in[c, ODD] + back_in[c, UP2] + back_in[c, DOWN2]
        pair2[c].start()

    def pair2_arrived(c):
        wait_exchange(PAIR2, c)
        gathered[c, y] = both_out[c] + both_in[c]
        for copy in gather[c]:
            copy.start()

    def gather_arrived(c):
        wait_exchange(GATHER, c)
        value = gathered[c].reshape(ANGLES * ZDEV, width)
        high = high_part(value)
        stack = jnp.concatenate([high, value - high, high, jnp.zeros_like(high)], axis=0).astype(BF16)
        update = jnp.dot(back_weights[...], stack, preferred_element_type=F32)
        updated_ref[:, c * width : (c + 1) * width] = vol[c] + update

    stages = (ray_sums, ray_arrived, pair_arrived, project, back_arrived, pair2_arrived, gather_arrived)
    forwarded = False
    done_tables = False
    done_update = False
    for stage, c in order_of_steps(chunks):
        if stage == 1 and not forwarded:
            wait_in(param_first)
            for copy in param_second:
                copy.start()
            forwarded = True
        if stage == 3 and not done_tables:
            load_measured.wait()
            tables()
            done_tables = True
        if stage == 4 and not done_update:
            update_weights()
            done_update = True
        stages[stage](c)

    for copy in param_first + param_second:
        copy.wait_send()
    for exchange in range(EXCHANGES):
        sent = vol.at[:, pl.ds(0, SENT_ROWS[exchange])]
        remote(sent, sent, exchange, 0, pair_dev).wait_send()


def body(volume, measured, foot_start, foot_len, order, ray_table):
    slices, share, columns = volume.shape
    cells = slices * share
    rows = measured.shape[1]
    flat = volume.reshape(cells, columns)
    chunks = CHUNKS
    width = columns // chunks
    vmem = pltpu.VMEM
    smem = pl.BlockSpec(memory_space=pltpu.SMEM)
    hbm = pl.BlockSpec(memory_space=pltpu.HBM)
    updated, residual = pl.pallas_call(
        functools.partial(exchange_kernel, chunks, width),
        out_shape=(
            jax.ShapeDtypeStruct((cells, columns), F32),
            jax.ShapeDtypeStruct((rows, columns), F32),
        ),
        in_specs=[smem, smem, hbm, hbm, hbm, hbm],
        out_specs=(pl.BlockSpec(memory_space=pltpu.VMEM),) * 2,
        scratch_shapes=[
            vmem((chunks, cells, width), F32),
            vmem((rows, columns), BF16),
            pltpu.SMEM(order.shape, jnp.int32),
            vmem(ray_table.shape, F32),
            vmem((chunks, 4, 2, ZDEV, width), F32),
            vmem((chunks, 3, 2, ZDEV, width), F32),
            vmem((chunks, 2, ZDEV, width), F32),
            vmem((chunks, 2, ZDEV, width), F32),
            vmem((chunks, 2, ZDEV, width), F32),
            vmem((chunks, 4, ZDEV, width), F32),
            vmem((chunks, 5, ZDEV, width), F32),
            vmem((chunks, 4, ZDEV, width), F32),
            vmem((chunks, 2, ZDEV, width), F32),
            vmem((chunks, 2, ZDEV, width), F32),
            vmem((chunks, 4, 2, ZDEV, width), F32),
            vmem((4, 2, 2, 8, 128), F32),
            vmem((4, 2, 8, 128), F32),
            vmem((ANGLES * ZDEV, cells), F32),
            vmem((ANGLES, ray_table.shape[1]), F32),
            vmem((rows, 128), BF16),
            vmem((48, 128), BF16),
            vmem((rows, 128), F32),
            vmem((cells, 4 * ANGLES * ZDEV), BF16),
            pltpu.SemaphoreType.DMA((chunks + 3,)),
            pltpu.SemaphoreType.DMA((EXCHANGES,)),
            pltpu.SemaphoreType.DMA((chunks, EXCHANGES)),
            pltpu.SemaphoreType.DMA((8,)),
            pltpu.SemaphoreType.DMA((8,)),
        ],
        compiler_params=pltpu.CompilerParams(
            collective_id=0, has_side_effects=True, vmem_limit_bytes=40 * 1024 * 1024
        ),
        name="exchange",
    )(
        foot_start, foot_len, *(
            pltpu.with_memory_space_constraint(a, pltpu.HBM)
            for a in (order, ray_table, flat, measured.reshape(rows, columns))
        )
    )
    return (updated.reshape(slices, share, columns), residual.reshape(measured.shape))


def solution(mesh):
    return jax.shard_map(
        body,
        mesh=mesh,
        in_specs=(
            P("slab", "ang", None),
            P("ang", "slab", None),
            P("slab", "ang"),
            P("slab", "ang"),
            P(),
            P(),
        ),
        out_specs=(P("slab", "ang", None), P("ang", "slab", None)),
        check_vma=False,
    )
```

```python
import functools

import jax
import jax.numpy as jnp
from jax import lax
from jax.experimental import pallas as pl
from jax.experimental.pallas import tpu as pltpu
from jax.sharding import PartitionSpec as P

ZDEV = 8
ANGLES = 8
WIDTHS = (512,) * 8
STORES = 8
LAG = 2.5
MESH = pl.DeviceIdType.MESH
F32 = jnp.float32
BF16 = jnp.bfloat16

SIB, ODD, UP2, DOWN2 = range(4)
BACK = (SIB, ODD, DOWN2, UP2)
FAR_FIRST = (UP2, DOWN2, ODD, SIB)
RAY, PAIR, SLAB, BACKPROJ, PAIR2, GATHER, EXCHANGES = range(7)
SENT_ROWS = (48, 16, 32, 32, 16, 48)


def order_of_steps(chunks):
    steps = [(k, c) for k in range(7) for c in range(chunks)]
    return sorted(steps, key=lambda step: (step[1] + LAG * step[0], -step[0]))


def hat(row, first, length, k):
    span = length / ZDEV
    centre = first + (k + 0.5) * span
    weight = jnp.maximum(0.0, 1.0 - jnp.abs(row + 0.5 - centre) / span)
    return jnp.where((row >= first) & (row < first + length), weight, 0.0)


def high_part(value):
    return value.astype(BF16).astype(F32)


def iota(shape, dim):
    return lax.broadcasted_iota(jnp.int32, shape, dim)


def exchange_kernel(
    widths,
    start_ref, length_ref, order_hbm, table_hbm, volume_hbm, measured_hbm,
    updated_ref, residual_ref,
    vol, meas, order_ref, table_ref, part, ray_in, pair_out, pair_in, sums, sums_in, back_out, back_in,
    both_out, both_in, gathered, params, neighbour_params, weights, picked,
    project_weights, spread_weights, scale, back_weights,
    load_sem, send_sem, recv_sem, psend_sem, precv_sem,
):
    chunks = len(widths)
    spans = [(sum(widths[:c]), sum(widths[: c + 1])) for c in range(chunks)]
    slab = lax.axis_index("slab")
    ang = lax.axis_index("ang")
    n_slab = lax.axis_size("slab")
    y = lax.rem(ang, 4)
    xl = ang // 4
    core = lax.rem(slab, 2)
    other = 1 - xl
    pair_dev = (slab, other * 4 + y)
    sib_dev = (slab + 1 - 2 * core, ang)
    odd_dev = (lax.rem(slab + 2 * core - 1 + n_slab, n_slab), other * 4 + y)
    up_dev = (lax.rem(slab + 2, n_slab), other * 4 + y)
    down_dev = (lax.rem(slab + n_slab - 2, n_slab), other * 4 + y)
    slab_devs = (sib_dev, odd_dev, up_dev, down_dev)
    y_of = [None] + [lax.rem(y + d, 4) for d in (1, 2, 3)]
    y_devs = [None] + [(slab, xl * 4 + y_of[d]) for d in (1, 2, 3)]

    def columns_of(ref, c, *index):
        begin, end = spans[c]
        index = index + (slice(None),) * (len(ref.shape) - 1 - len(index))
        return ref.at[index + (pl.ds(begin, end - begin),)]

    load_order = pltpu.make_async_copy(order_hbm, order_ref, load_sem.at[chunks + 2])
    load_order.start()
    load_table = pltpu.make_async_copy(table_hbm, table_ref, load_sem.at[chunks + 1])
    load_table.start()
    loads = [
        pltpu.make_async_copy(columns_of(volume_hbm, c), columns_of(vol, c), load_sem.at[c])
        for c in range(chunks)
    ]
    for copy in loads[:2]:
        copy.start()
    load_measured = pltpu.make_async_copy(measured_hbm, meas, load_sem.at[chunks])
    barrier = pltpu.get_barrier_semaphore()
    greeted = (*y_devs[1:], pair_dev, *slab_devs)
    for device in greeted:
        pl.semaphore_signal(barrier, inc=1, device_id=device, device_id_type=MESH)

    first_here = jnp.full((8, 128), start_ref[0, 0], jnp.int32).astype(F32)
    length_here = jnp.full((8, 128), length_ref[0, 0], jnp.int32).astype(F32)
    params[y, xl, 0] = first_here
    params[y, xl, 1] = length_here

    load_order.wait()
    load_table.wait()
    for copy in loads[2:]:
        copy.start()
    load_measured.start()
    for m in range(ANGLES):
        angle = (m % 2) * 4 + m // 2
        picked[pl.ds(m, 1), :] = table_ref[pl.ds(order_ref[angle], 1), :]
    cells = picked.shape[1]
    share = cells // 8
    pick = (iota((cells, cells), 0) == ang * share + lax.rem(iota((cells, cells), 1), share)).astype(F32)
    mine = jnp.dot(picked[...], pick, precision=lax.Precision.HIGHEST, preferred_element_type=F32)
    blocks = jnp.broadcast_to(mine[:, None, :], (ANGLES, ZDEV, cells)).reshape(ANGLES * ZDEV, cells)
    own_slice = lax.rem(iota(blocks.shape, 0), ZDEV) == iota(blocks.shape, 1) // share
    blocks = jnp.where(own_slice, blocks, 0.0)
    weights[...] = blocks
    blocks_high = high_part(blocks)
    ray_weights = jnp.concatenate([blocks_high, blocks - blocks_high], axis=0).astype(BF16)

    def partial_sums(c):
        loads[c].wait()
        value = columns_of(vol, c)[...]
        high = value.astype(BF16)
        low = (value - high.astype(F32)).astype(BF16)
        first = jnp.dot(ray_weights, high, preferred_element_type=F32)
        second = jnp.dot(ray_weights[: ANGLES * ZDEV], low, preferred_element_type=F32)
        total = first[: ANGLES * ZDEV] + first[ANGLES * ZDEV :] + second
        columns_of(part, c)[...] = total.reshape(*part.shape[:-1], -1)
    partial_sums(0)
    pl.semaphore_wait(barrier, len(greeted))

    def remote(src, dst, exchange, c, device):
        return pltpu.make_async_remote_copy(
            src_ref=src, dst_ref=dst, send_sem=send_sem.at[exchange], recv_sem=recv_sem.at[c, exchange],
            device_id=device, device_id_type=MESH,
        )

    def param_copy(src, dst, k, device):
        return pltpu.make_async_remote_copy(
            src_ref=src, dst_ref=dst, send_sem=psend_sem.at[k], recv_sem=precv_sem.at[k],
            device_id=device, device_id_type=MESH,
        )

    own_params = params.at[y, xl]
    param_first = [
        param_copy(own_params, own_params, 0, pair_dev),
        param_copy(own_params, neighbour_params.at[SIB], 1, sib_dev),
    ]
    param_second = [
        param_copy(params.at[y, other], neighbour_params.at[ODD], 2, odd_dev),
        param_copy(params.at[y, other], neighbour_params.at[DOWN2], 3, up_dev),
        param_copy(params.at[y, other], neighbour_params.at[UP2], 4, down_dev),
    ] + [param_copy(params.at[y], params.at[y], 4 + d, y_devs[d]) for d in (1, 2, 3)]
    for copy in param_first:
        copy.start()

    ray = [[remote(columns_of(part, c, y_of[d]), columns_of(ray_in, c, d - 1), RAY, c, y_devs[d]) for d in (2, 1, 3)] for c in range(chunks)]
    pair = [remote(columns_of(pair_out, c), columns_of(pair_in, c), PAIR, c, pair_dev) for c in range(chunks)]
    to_slab = [
        [remote(columns_of(sums, c, xl if k == SIB else other), columns_of(sums_in, c, BACK[k]), SLAB, c, slab_devs[k]) for k in FAR_FIRST]
        for c in range(chunks)
    ]
    to_back = [
        [remote(columns_of(back_out, c, 1 + k), columns_of(back_in, c, BACK[k]), BACKPROJ, c, slab_devs[k]) for k in FAR_FIRST]
        for c in range(chunks)
    ]
    pair2 = [remote(columns_of(both_out, c), columns_of(both_in, c), PAIR2, c, pair_dev) for c in range(chunks)]
    gather = [[remote(columns_of(gathered, c, y), columns_of(gathered, c, y), GATHER, c, y_devs[d]) for d in (2, 1, 3)] for c in range(chunks)]
    landing = (ray_in, pair_in, sums_in, back_in, both_in, gathered)

    def wait_in(copies):
        for copy in copies:
            copy.wait_recv()

    def wait_exchange(exchange, c):
        whole = columns_of(landing[exchange], c, *((pl.ds(0, 3),) if exchange == GATHER else ()))
        remote(whole, whole, exchange, c, pair_dev).wait_recv()

    def tables():
        wait_in(param_second)
        tiles = [params[y, xl]] + [neighbour_params[k] for k in range(4)]
        rows = first_here.shape[0] * 4
        lane = iota((rows, 128), 1)
        row = (slab * rows + iota((rows, 128), 0)).astype(F32)
        third = (lane >= 40).astype(jnp.int32) + (lane >= 80).astype(jnp.int32) + (lane >= 120).astype(jnp.int32)
        within = lane - 40 * third
        role = lax.shift_right_logical(within, 3)
        first = jnp.zeros((rows, 128), F32)
        length = jnp.full((rows, 128), 32.0, F32)
        for k in range(5):
            first = jnp.where(role == k, tiles[k][0, 0:1, :], first)
            length = jnp.where(role == k, tiles[k][1, 0:1, :], length)
        weight = hat(row, first, length, lax.bitwise_and(within, 7).astype(F32))
        high = high_part(weight)
        project_weights[...] = jnp.where(third < 2, high, jnp.where(third == 2, weight - high, 0.0)).astype(BF16)
        coverage = jnp.sum(jnp.where(third == 0, weight, 0.0), axis=1, keepdims=True)
        path = jnp.sum(table_ref[pl.ds(order_ref[ang], 1), :], axis=1, keepdims=True)
        scale[...] = jnp.broadcast_to(1.0 / jnp.maximum(path * coverage, 0.25), scale.shape)
        lane = iota((8, 128), 1)
        quarter = lax.shift_right_logical(lane, 5)
        row = (slab * rows + lax.bitwise_and(lane, 31)).astype(F32)
        k8 = iota((8, 128), 0).astype(F32)
        spread = []
        for k in range(5):
            weight = hat(row, tiles[k][0], tiles[k][1], k8)
            high = high_part(weight)
            spread.append(jnp.where(quarter < 2, high, jnp.where(quarter == 2, weight - high, 0.0)))
        spread.append(jnp.zeros((8, 128), F32))
        spread_weights[...] = jnp.concatenate(spread, axis=0).astype(BF16)

    def update_weights():
        lane = iota((8, 128), 1)
        base = (slab - 2) * 32
        k8 = iota((8, 128), 0).astype(F32)
        column = jnp.zeros((8, cells), F32)
        for m in range(ANGLES):
            tile_first, tile_length = params[m // 2, m % 2, 0], params[m // 2, m % 2, 1]
            near = hat((base + lane).astype(F32), tile_first, tile_length, k8)
            far = hat((base + 128 + lane).astype(F32), tile_first, tile_length, k8)
            slice_weight = jnp.sum(near + far, axis=1, keepdims=True)
            column = column + weights[m * 8 : m * 8 + 8, :] * slice_weight
        column = jnp.sum(column, axis=0, keepdims=True)
        ratio = weights[...] / column
        high = high_part(ratio)
        stack = jnp.concatenate([high, high, ratio - high, jnp.zeros_like(high)], axis=0)
        back_weights[...] = stack.T.astype(BF16)

    def ray_sums(c):
        if c:
            partial_sums(c)
        for copy in ray[c]:
            copy.start()

    def ray_arrived(c):
        wait_exchange(RAY, c)
        arrived = columns_of(ray_in, c)[...]
        columns_of(pair_out, c)[...] = columns_of(part, c, y)[...] + arrived[0] + arrived[1] + arrived[2]
        pair[c].start()

    def pair_arrived(c):
        wait_exchange(PAIR, c)
        columns_of(sums, c)[...] = columns_of(pair_out, c)[...] + columns_of(pair_in, c)[...]
        for copy in to_slab[c]:
            copy.start()

    def project(c):
        wait_exchange(SLAB, c)
        five = jnp.concatenate([columns_of(sums, c, xl)[...]] + [columns_of(sums_in, c, k)[...] for k in range(4)], axis=0)
        high = high_part(five)
        stack = jnp.concatenate([high, five - high, high, jnp.zeros_like(high[:8])], axis=0).astype(BF16)
        projected = jnp.dot(project_weights[...], stack, preferred_element_type=F32)
        here = (columns_of(meas, c)[...].astype(F32) - projected) * scale[:, 0:1]
        columns_of(residual_ref, c)[...] = here
        high = high_part(here)
        stack = jnp.concatenate([high, here - high, high, jnp.zeros_like(high)], axis=0).astype(BF16)
        spread = jnp.dot(spread_weights[...], stack, preferred_element_type=F32)
        columns_of(back_out, c)[...] = spread[:40].reshape(*back_out.shape[:-1], -1)
        for copy in to_back[c]:
            copy.start()

    def back_arrived(c):
        wait_exchange(BACKPROJ, c)
        arrived = columns_of(back_in, c)[...]
        columns_of(both_out, c, xl)[...] = columns_of(back_out, c, 0)[...] + arrived[SIB]
        columns_of(both_out, c, other)[...] = arrived[ODD] + arrived[UP2] + arrived[DOWN2]
        pair2[c].start()

    def pair2_arrived(c):
        wait_exchange(PAIR2, c)
        columns_of(gathered, c, y)[...] = columns_of(both_out, c)[...] + columns_of(both_in, c)[...]
        for copy in gather[c]:
            copy.start()

    def gather_arrived(c):
        wait_exchange(GATHER, c)
        value = columns_of(gathered, c)[...].reshape(ANGLES * ZDEV, -1)
        high = high_part(value)
        stack = jnp.concatenate([high, value - high, high, jnp.zeros_like(high)], axis=0).astype(BF16)
        update = jnp.dot(back_weights[...], stack, preferred_element_type=F32)
        columns_of(updated_ref, c)[...] = columns_of(vol, c)[...] + update

    stages = (ray_sums, ray_arrived, pair_arrived, project, back_arrived, pair2_arrived, gather_arrived)
    forwarded = False
    done_tables = False
    done_update = False
    for stage, c in order_of_steps(chunks):
        if stage == 1 and not forwarded:
            wait_in(param_first)
            for copy in param_second:
                copy.start()
            forwarded = True
        stages[stage](c)
        if stage == 2 and not done_tables:
            load_measured.wait()
            tables()
            done_tables = True
        if stage == 3 and not done_update:
            update_weights()
            done_update = True

    for copy in param_first + param_second:
        copy.wait_send()
    for exchange in range(EXCHANGES):
        sent = vol.at[pl.ds(0, SENT_ROWS[exchange])]
        remote(sent, sent, exchange, 0, pair_dev).wait_send()


def store_kernel(updated_ref, residual_ref, updated_hbm, residual_hbm, sem):
    cells = updated_ref.shape[0]
    step = cells // STORES
    copies = [
        pltpu.make_async_copy(updated_ref.at[pl.ds(k * step, step)], updated_hbm.at[pl.ds(k * step, step)], sem.at[k])
        for k in range(STORES)
    ]
    copies.append(pltpu.make_async_copy(residual_ref, residual_hbm, sem.at[STORES]))
    for copy in copies:
        copy.start()
    for copy in copies:
        copy.wait()


def body(volume, measured, foot_start, foot_len, order, ray_table):
    slices, share, columns = volume.shape
    cells = slices * share
    rows = measured.shape[1]
    flat = volume.reshape(cells, columns)
    chunks = len(WIDTHS)
    vmem = pltpu.VMEM
    smem = pl.BlockSpec(memory_space=pltpu.SMEM)
    hbm = pl.BlockSpec(memory_space=pltpu.HBM)
    updated, residual = pl.pallas_call(
        functools.partial(exchange_kernel, WIDTHS),
        out_shape=(
            jax.ShapeDtypeStruct((cells, columns), F32),
            jax.ShapeDtypeStruct((rows, columns), F32),
        ),
        in_specs=[smem, smem, hbm, hbm, hbm, hbm],
        out_specs=(pl.BlockSpec(memory_space=pltpu.VMEM),) * 2,
        scratch_shapes=[
            vmem((cells, columns), F32),
            vmem((rows, columns), BF16),
            pltpu.SMEM(order.shape, jnp.int32),
            vmem(ray_table.shape, F32),
            vmem((4, 2, ZDEV, columns), F32),
            vmem((3, 2, ZDEV, columns), F32),
            vmem((2, ZDEV, columns), F32),
            vmem((2, ZDEV, columns), F32),
            vmem((2, ZDEV, columns), F32),
            vmem((4, ZDEV, columns), F32),
            vmem((5, ZDEV, columns), F32),
            vmem((4, ZDEV, columns), F32),
            vmem((2, ZDEV, columns), F32),
            vmem((2, ZDEV, columns), F32),
            vmem((4, 2, ZDEV, columns), F32),
            vmem((4, 2, 2, 8, 128), F32),
            vmem((4, 2, 8, 128), F32),
            vmem((ANGLES * ZDEV, cells), F32),
            vmem((ANGLES, ray_table.shape[1]), F32),
            vmem((rows, 128), BF16),
            vmem((48, 128), BF16),
            vmem((rows, 128), F32),
            vmem((cells, 4 * ANGLES * ZDEV), BF16),
            pltpu.SemaphoreType.DMA((chunks + 3,)),
            pltpu.SemaphoreType.DMA((EXCHANGES,)),
            pltpu.SemaphoreType.DMA((chunks, EXCHANGES)),
            pltpu.SemaphoreType.DMA((8,)),
            pltpu.SemaphoreType.DMA((8,)),
        ],
        compiler_params=pltpu.CompilerParams(
            collective_id=0, has_side_effects=True, vmem_limit_bytes=40 * 1024 * 1024
        ),
        name="exchange",
    )(
        foot_start, foot_len, *(
            pltpu.with_memory_space_constraint(a, pltpu.HBM)
            for a in (order, ray_table, flat, measured.reshape(rows, columns))
        )
    )
    whole = pl.BlockSpec(memory_space=pltpu.VMEM)
    updated, residual = pl.pallas_call(
        store_kernel,
        out_shape=(
            jax.ShapeDtypeStruct((cells, columns), F32),
            jax.ShapeDtypeStruct((rows, columns), F32),
        ),
        in_specs=[whole, whole],
        out_specs=(hbm, hbm),
        scratch_shapes=[pltpu.SemaphoreType.DMA((STORES + 1,))],
        compiler_params=pltpu.CompilerParams(vmem_limit_bytes=1024 * 1024),
        name="store",
    )(updated, residual)
    return (updated.reshape(slices, share, columns), residual.reshape(measured.shape))


def solution(mesh):
    return jax.shard_map(
        body,
        mesh=mesh,
        in_specs=(
            P("slab", "ang", None),
            P("ang", "slab", None),
            P("slab", "ang"),
            P("slab", "ang"),
            P(),
            P(),
        ),
        out_specs=(P("slab", "ang", None), P("ang", "slab", None)),
        check_vma=False,
    )
```

```python
import functools

import jax
import jax.numpy as jnp
from jax import lax
from jax.experimental import pallas as pl
from jax.experimental.pallas import tpu as pltpu
from jax.sharding import PartitionSpec as P

ZDEV = 8
ANGLES = 8
WIDTHS = (512,) * 8
STORES = 8
LAG = 2.5
MESH = pl.DeviceIdType.MESH
F32 = jnp.float32
BF16 = jnp.bfloat16

SIB, ODD, UP2, DOWN2 = range(4)
BACK = (SIB, ODD, DOWN2, UP2)
FAR_FIRST = (UP2, DOWN2, ODD, SIB)
RAY, PAIR, SLAB, BACKPROJ, PAIR2, GATHER, EXCHANGES = range(7)
SENT_ROWS = (48, 16, 32, 32, 16, 48)


def order_of_steps(chunks):
    steps = [(k, c) for k in range(7) for c in range(chunks)]
    return sorted(steps, key=lambda step: (step[1] + LAG * step[0], -step[0]))


def hat(row, first, length, k):
    span = length / ZDEV
    centre = first + (k + 0.5) * span
    weight = jnp.maximum(0.0, 1.0 - jnp.abs(row + 0.5 - centre) / span)
    return jnp.where((row >= first) & (row < first + length), weight, 0.0)


def high_part(value):
    return value.astype(BF16).astype(F32)


def iota(shape, dim):
    return lax.broadcasted_iota(jnp.int32, shape, dim)


def exchange_kernel(
    widths,
    start_ref, length_ref, order_hbm, table_hbm, volume_hbm, measured_hbm,
    updated_ref, residual_ref,
    vol, meas, order_ref, table_ref, part, ray_in, pair_out, pair_in, sums, sums_in, back_out, back_in,
    both_out, both_in, gathered, params, neighbour_params, weights, picked,
    project_weights, spread_weights, scale, back_weights,
    load_sem, send_sem, recv_sem, psend_sem, precv_sem,
):
    chunks = len(widths)
    spans = [(sum(widths[:c]), sum(widths[: c + 1])) for c in range(chunks)]
    slab = lax.axis_index("slab")
    ang = lax.axis_index("ang")
    n_slab = lax.axis_size("slab")
    y = lax.rem(ang, 4)
    xl = ang // 4
    core = lax.rem(slab, 2)
    other = 1 - xl
    pair_dev = (slab, other * 4 + y)
    sib_dev = (slab + 1 - 2 * core, ang)
    odd_dev = (lax.rem(slab + 2 * core - 1 + n_slab, n_slab), other * 4 + y)
    up_dev = (lax.rem(slab + 2, n_slab), other * 4 + y)
    down_dev = (lax.rem(slab + n_slab - 2, n_slab), other * 4 + y)
    slab_devs = (sib_dev, odd_dev, up_dev, down_dev)
    y_of = [None] + [lax.rem(y + d, 4) for d in (1, 2, 3)]
    y_devs = [None] + [(slab, xl * 4 + y_of[d]) for d in (1, 2, 3)]

    def columns_of(ref, c, *index):
        begin, end = spans[c]
        index = index + (slice(None),) * (len(ref.shape) - 1 - len(index))
        return ref.at[index + (pl.ds(begin, end - begin),)]

    barrier = pltpu.get_barrier_semaphore()
    greeted = (*y_devs[1:], pair_dev, *slab_devs)
    for device in greeted:
        pl.semaphore_signal(barrier, inc=1, device_id=device, device_id_type=MESH)

    load_order = pltpu.make_async_copy(order_hbm, order_ref, load_sem.at[chunks + 2])
    load_order.start()
    load_table = pltpu.make_async_copy(table_hbm, table_ref, load_sem.at[chunks + 1])
    load_table.start()
    loads = [
        pltpu.make_async_copy(columns_of(volume_hbm, c), columns_of(vol, c), load_sem.at[c])
        for c in range(chunks)
    ]
    for copy in loads[:2]:
        copy.start()
    load_measured = pltpu.make_async_copy(measured_hbm, meas, load_sem.at[chunks])
    first_here = jnp.full((8, 128), start_ref[0, 0], jnp.int32).astype(F32)
    length_here = jnp.full((8, 128), length_ref[0, 0], jnp.int32).astype(F32)
    params[y, xl, 0] = first_here
    params[y, xl, 1] = length_here

    load_order.wait()
    load_table.wait()
    for copy in loads[2:]:
        copy.start()
    load_measured.start()
    for m in range(ANGLES):
        angle = (m % 2) * 4 + m // 2
        picked[pl.ds(m, 1), :] = table_ref[pl.ds(order_ref[angle], 1), :]
    cells = picked.shape[1]
    share = cells // 8
    pick = (iota((cells, cells), 0) == ang * share + lax.rem(iota((cells, cells), 1), share)).astype(BF16)
    chosen = picked[...]
    high = high_part(chosen)
    middle = high_part(chosen - high)
    parts = jnp.concatenate([high, middle, chosen - high - middle, jnp.zeros_like(high)], axis=0).astype(BF16)
    parts = jnp.dot(parts, pick, preferred_element_type=F32)
    mine = parts[:ANGLES] + parts[ANGLES : 2 * ANGLES] + parts[2 * ANGLES : 3 * ANGLES]
    blocks = jnp.broadcast_to(mine[:, None, :], (ANGLES, ZDEV, cells)).reshape(ANGLES * ZDEV, cells)
    own_slice = lax.rem(iota(blocks.shape, 0), ZDEV) == iota(blocks.shape, 1) // share
    blocks = jnp.where(own_slice, blocks, 0.0)
    weights[...] = blocks
    blocks_high = high_part(blocks)
    ray_weights = jnp.concatenate([blocks_high, blocks - blocks_high], axis=0).astype(BF16)

    def partial_sums(c):
        loads[c].wait()
        value = columns_of(vol, c)[...]
        high = value.astype(BF16)
        low = (value - high.astype(F32)).astype(BF16)
        first = jnp.dot(ray_weights, high, preferred_element_type=F32)
        second = jnp.dot(ray_weights[: ANGLES * ZDEV], low, preferred_element_type=F32)
        total = first[: ANGLES * ZDEV] + first[ANGLES * ZDEV :] + second
        columns_of(part, c)[...] = total.reshape(*part.shape[:-1], -1)
    partial_sums(0)
    pl.semaphore_wait(barrier, len(greeted))

    def remote(src, dst, exchange, c, device):
        return pltpu.make_async_remote_copy(
            src_ref=src, dst_ref=dst, send_sem=send_sem.at[exchange], recv_sem=recv_sem.at[c, exchange],
            device_id=device, device_id_type=MESH,
        )

    def param_copy(src, dst, k, device):
        return pltpu.make_async_remote_copy(
            src_ref=src, dst_ref=dst, send_sem=psend_sem.at[k], recv_sem=precv_sem.at[k],
            device_id=device, device_id_type=MESH,
        )

    own_params = params.at[y, xl]
    param_first = [
        param_copy(own_params, own_params, 0, pair_dev),
        param_copy(own_params, neighbour_params.at[SIB], 1, sib_dev),
    ]
    param_second = [
        param_copy(params.at[y, other], neighbour_params.at[ODD], 2, odd_dev),
        param_copy(params.at[y, other], neighbour_params.at[DOWN2], 3, up_dev),
        param_copy(params.at[y, other], neighbour_params.at[UP2], 4, down_dev),
    ] + [param_copy(params.at[y], params.at[y], 4 + d, y_devs[d]) for d in (1, 2, 3)]
    for copy in param_first:
        copy.start()

    ray = [[remote(columns_of(part, c, y_of[d]), columns_of(ray_in, c, d - 1), RAY, c, y_devs[d]) for d in (2, 1, 3)] for c in range(chunks)]
    pair = [remote(columns_of(pair_out, c), columns_of(pair_in, c), PAIR, c, pair_dev) for c in range(chunks)]
    to_slab = [
        [remote(columns_of(sums, c, xl if k == SIB else other), columns_of(sums_in, c, BACK[k]), SLAB, c, slab_devs[k]) for k in FAR_FIRST]
        for c in range(chunks)
    ]
    to_back = [
        [remote(columns_of(back_out, c, 1 + k), columns_of(back_in, c, BACK[k]), BACKPROJ, c, slab_devs[k]) for k in FAR_FIRST]
        for c in range(chunks)
    ]
    pair2 = [remote(columns_of(both_out, c), columns_of(both_in, c), PAIR2, c, pair_dev) for c in range(chunks)]
    gather = [[remote(columns_of(gathered, c, y), columns_of(gathered, c, y), GATHER, c, y_devs[d]) for d in (2, 1, 3)] for c in range(chunks)]
    landing = (ray_in, pair_in, sums_in, back_in, both_in, gathered)

    def wait_in(copies):
        for copy in copies:
            copy.wait_recv()

    def wait_exchange(exchange, c):
        whole = columns_of(landing[exchange], c, *((pl.ds(0, 3),) if exchange == GATHER else ()))
        remote(whole, whole, exchange, c, pair_dev).wait_recv()

    def tables():
        wait_in(param_second)
        tiles = [params[y, xl]] + [neighbour_params[k] for k in range(4)]
        rows = first_here.shape[0] * 4
        lane = iota((rows, 128), 1)
        row = (slab * rows + iota((rows, 128), 0)).astype(F32)
        third = (lane >= 40).astype(jnp.int32) + (lane >= 80).astype(jnp.int32) + (lane >= 120).astype(jnp.int32)
        within = lane - 40 * third
        role = lax.shift_right_logical(within, 3)
        first = jnp.zeros((rows, 128), F32)
        length = jnp.full((rows, 128), 32.0, F32)
        for k in range(5):
            first = jnp.where(role == k, tiles[k][0, 0:1, :], first)
            length = jnp.where(role == k, tiles[k][1, 0:1, :], length)
        weight = hat(row, first, length, lax.bitwise_and(within, 7).astype(F32))
        high = high_part(weight)
        project_weights[...] = jnp.where(third < 2, high, jnp.where(third == 2, weight - high, 0.0)).astype(BF16)
        coverage = jnp.sum(jnp.where(third == 0, weight, 0.0), axis=1, keepdims=True)
        path = jnp.sum(table_ref[pl.ds(order_ref[ang], 1), :], axis=1, keepdims=True)
        scale[...] = jnp.broadcast_to(1.0 / jnp.maximum(path * coverage, 0.25), scale.shape)
        lane = iota((8, 128), 1)
        quarter = lax.shift_right_logical(lane, 5)
        row = (slab * rows + lax.bitwise_and(lane, 31)).astype(F32)
        k8 = iota((8, 128), 0).astype(F32)
        spread = []
        for k in range(5):
            weight = hat(row, tiles[k][0], tiles[k][1], k8)
            high = high_part(weight)
            spread.append(jnp.where(quarter < 2, high, jnp.where(quarter == 2, weight - high, 0.0)))
        spread.append(jnp.zeros((8, 128), F32))
        spread_weights[...] = jnp.concatenate(spread, axis=0).astype(BF16)

    def update_weights():
        lane = iota((8, 128), 1)
        base = (slab - 2) * 32
        k8 = iota((8, 128), 0).astype(F32)
        column = jnp.zeros((8, cells), F32)
        for m in range(ANGLES):
            tile_first, tile_length = params[m // 2, m % 2, 0], params[m // 2, m % 2, 1]
            near = hat((base + lane).astype(F32), tile_first, tile_length, k8)
            far = hat((base + 128 + lane).astype(F32), tile_first, tile_length, k8)
            slice_weight = jnp.sum(near + far, axis=1, keepdims=True)
            column = column + weights[m * 8 : m * 8 + 8, :] * slice_weight
        column = jnp.sum(column, axis=0, keepdims=True)
        ratio = weights[...] / column
        high = high_part(ratio)
        stack = jnp.concatenate([high, high, ratio - high, jnp.zeros_like(high)], axis=0)
        back_weights[...] = stack.T.astype(BF16)

    def ray_sums(c):
        if c:
            partial_sums(c)
        for copy in ray[c]:
            copy.start()

    def ray_arrived(c):
        wait_exchange(RAY, c)
        arrived = columns_of(ray_in, c)[...]
        columns_of(pair_out, c)[...] = columns_of(part, c, y)[...] + arrived[0] + arrived[1] + arrived[2]
        pair[c].start()

    def pair_arrived(c):
        wait_exchange(PAIR, c)
        columns_of(sums, c)[...] = columns_of(pair_out, c)[...] + columns_of(pair_in, c)[...]
        for copy in to_slab[c]:
            copy.start()

    def project(c):
        wait_exchange(SLAB, c)
        five = jnp.concatenate([columns_of(sums, c, xl)[...]] + [columns_of(sums_in, c, k)[...] for k in range(4)], axis=0)
        high = high_part(five)
        stack = jnp.concatenate([high, five - high, high, jnp.zeros_like(high[:8])], axis=0).astype(BF16)
        projected = jnp.dot(project_weights[...], stack, preferred_element_type=F32)
        here = (columns_of(meas, c)[...].astype(F32) - projected) * scale[:, 0:1]
        columns_of(residual_ref, c)[...] = here
        high = high_part(here)
        stack = jnp.concatenate([high, here - high, high, jnp.zeros_like(high)], axis=0).astype(BF16)
        spread = jnp.dot(spread_weights[...], stack, preferred_element_type=F32)
        columns_of(back_out, c)[...] = spread[:40].reshape(*back_out.shape[:-1], -1)
        for copy in to_back[c]:
            copy.start()

    def back_arrived(c):
        wait_exchange(BACKPROJ, c)
        arrived = columns_of(back_in, c)[...]
        columns_of(both_out, c, xl)[...] = columns_of(back_out, c, 0)[...] + arrived[SIB]
        columns_of(both_out, c, other)[...] = arrived[ODD] + arrived[UP2] + arrived[DOWN2]
        pair2[c].start()

    def pair2_arrived(c):
        wait_exchange(PAIR2, c)
        columns_of(gathered, c, y)[...] = columns_of(both_out, c)[...] + columns_of(both_in, c)[...]
        for copy in gather[c]:
            copy.start()

    def gather_arrived(c):
        wait_exchange(GATHER, c)
        value = columns_of(gathered, c)[...].reshape(ANGLES * ZDEV, -1)
        high = high_part(value)
        stack = jnp.concatenate([high, value - high, high, jnp.zeros_like(high)], axis=0).astype(BF16)
        update = jnp.dot(back_weights[...], stack, preferred_element_type=F32)
        columns_of(updated_ref, c)[...] = columns_of(vol, c)[...] + update

    stages = (ray_sums, ray_arrived, pair_arrived, project, back_arrived, pair2_arrived, gather_arrived)
    forwarded = False
    done_tables = False
    done_update = False
    for stage, c in order_of_steps(chunks):
        if stage == 1 and not forwarded:
            wait_in(param_first)
            for copy in param_second:
                copy.start()
            forwarded = True
        stages[stage](c)
        if stage == 2 and not done_tables:
            load_measured.wait()
            tables()
            done_tables = True
        if stage == 3 and not done_update:
            update_weights()
            done_update = True

    for copy in param_first + param_second:
        copy.wait_send()
    for exchange in range(EXCHANGES):
        sent = vol.at[pl.ds(0, SENT_ROWS[exchange])]
        remote(sent, sent, exchange, 0, pair_dev).wait_send()


def store_kernel(updated_ref, residual_ref, updated_hbm, residual_hbm, sem):
    cells = updated_ref.shape[0]
    step = cells // STORES
    copies = [
        pltpu.make_async_copy(updated_ref.at[pl.ds(k * step, step)], updated_hbm.at[pl.ds(k * step, step)], sem.at[k])
        for k in range(STORES)
    ]
    copies.append(pltpu.make_async_copy(residual_ref, residual_hbm, sem.at[STORES]))
    for copy in copies:
        copy.start()
    for copy in copies:
        copy.wait()


def body(volume, measured, foot_start, foot_len, order, ray_table):
    slices, share, columns = volume.shape
    cells = slices * share
    rows = measured.shape[1]
    flat = volume.reshape(cells, columns)
    chunks = len(WIDTHS)
    vmem = pltpu.VMEM
    smem = pl.BlockSpec(memory_space=pltpu.SMEM)
    hbm = pl.BlockSpec(memory_space=pltpu.HBM)
    updated, residual = pl.pallas_call(
        functools.partial(exchange_kernel, WIDTHS),
        out_shape=(
            jax.ShapeDtypeStruct((cells, columns), F32),
            jax.ShapeDtypeStruct((rows, columns), F32),
        ),
        in_specs=[smem, smem, hbm, hbm, hbm, hbm],
        out_specs=(pl.BlockSpec(memory_space=pltpu.VMEM),) * 2,
        scratch_shapes=[
            vmem((cells, columns), F32),
            vmem((rows, columns), BF16),
            pltpu.SMEM(order.shape, jnp.int32),
            vmem(ray_table.shape, F32),
            vmem((4, 2, ZDEV, columns), F32),
            vmem((3, 2, ZDEV, columns), F32),
            vmem((2, ZDEV, columns), F32),
            vmem((2, ZDEV, columns), F32),
            vmem((2, ZDEV, columns), F32),
            vmem((4, ZDEV, columns), F32),
            vmem((5, ZDEV, columns), F32),
            vmem((4, ZDEV, columns), F32),
            vmem((2, ZDEV, columns), F32),
            vmem((2, ZDEV, columns), F32),
            vmem((4, 2, ZDEV, columns), F32),
            vmem((4, 2, 2, 8, 128), F32),
            vmem((4, 2, 8, 128), F32),
            vmem((ANGLES * ZDEV, cells), F32),
            vmem((ANGLES, ray_table.shape[1]), F32),
            vmem((rows, 128), BF16),
            vmem((48, 128), BF16),
            vmem((rows, 128), F32),
            vmem((cells, 4 * ANGLES * ZDEV), BF16),
            pltpu.SemaphoreType.DMA((chunks + 3,)),
            pltpu.SemaphoreType.DMA((EXCHANGES,)),
            pltpu.SemaphoreType.DMA((chunks, EXCHANGES)),
            pltpu.SemaphoreType.DMA((8,)),
            pltpu.SemaphoreType.DMA((8,)),
        ],
        compiler_params=pltpu.CompilerParams(
            collective_id=0, has_side_effects=True, vmem_limit_bytes=40 * 1024 * 1024
        ),
        name="exchange",
    )(
        foot_start, foot_len, *(
            pltpu.with_memory_space_constraint(a, pltpu.HBM)
            for a in (order, ray_table, flat, measured.reshape(rows, columns))
        )
    )
    whole = pl.BlockSpec(memory_space=pltpu.VMEM)
    updated, residual = pl.pallas_call(
        store_kernel,
        out_shape=(
            jax.ShapeDtypeStruct((cells, columns), F32),
            jax.ShapeDtypeStruct((rows, columns), F32),
        ),
        in_specs=[whole, whole],
        out_specs=(hbm, hbm),
        scratch_shapes=[pltpu.SemaphoreType.DMA((STORES + 1,))],
        compiler_params=pltpu.CompilerParams(vmem_limit_bytes=1024 * 1024),
        name="store",
    )(updated, residual)
    return (updated.reshape(slices, share, columns), residual.reshape(measured.shape))


def solution(mesh):
    return jax.shard_map(
        body,
        mesh=mesh,
        in_specs=(
            P("slab", "ang", None),
            P("ang", "slab", None),
            P("slab", "ang"),
            P("slab", "ang"),
            P(),
            P(),
        ),
        out_specs=(P("slab", "ang", None), P("ang", "slab", None)),
        check_vma=False,
    )
```
